256 devices in a mesh: role: 4 (over z_lo), grp: 4 (over z_hi, core), run: 16 (over y, x).
Axes of the slice: x: 4, y: 4, z: 8 (z_hi: 2, z_lo: 4; z = z_hi * 4 + z_lo), core: 2. Of those that a mesh axis runs over, the one named last changes fastest.
Arguments:
- prior_fields: float32 [1024, 3, 256, 128], P(('role', 'grp'), None, 'run'), may hold values from -0.4 to 1.4, as said below
- measured_point_location: int32 [4096], P('run'), may hold values from 0 to 2047
- measured_depths: float32 [4096], P('run'), may hold values from 0.7 to 1.3
- inverse_noise_deviation: float32 [4096], P('run'), may hold values from 5 to 40
- sample_noise_draw: float32 [1024, 4096], P(None, 'run'), may hold values from -6 to 6
- sample_line_labels: int32 [1024], P(('role', 'grp')), may hold values from 0 to 1023, each once
Outputs:
- analysis: float32 [1024, 3, 256, 128], P(('role', 'grp'), None, 'run')
The draws below stay inside these ranges and needn't reach their ends.
Inputs may be any that keep to these rules, and one draw needn't show every extreme that they name: `prior_fields`: the depth component (index 0 of the second dimension) lies within 0.75 to 1.4, the momenta within -0.4 to 0.4.
All inputs are finite; a program needn't handle non-finite values.
Results may differ from the reference program's by a relative error of at most 0.0003.
Values sent between devices are 32-bit elements; how exact they have to be, the bound alone decides.
No kernel may reach another device: no remote copies, remote signals or barrier semaphores. Data moves between devices by JAX's collectives and lax.ppermute only.
A program may use at most 64 MiB of HBM per device.

```python
import math
import jax
import jax.numpy as jnp
from jax import lax

ENSEMBLE_SIZE = 1024
POINTS_ACROSS = 128
RY = 16
OBS_DEV = 256
STEPS = 4
CHEB = 8
LATTICE_LINES = 256
NOBS = 4096


def draw_prior_fields(key, part):
    keys = jax.random.split(jax.random.fold_in(key, 7), 2)
    depth = 1.0 + 0.25 * jax.random.uniform(keys[0], (ENSEMBLE_SIZE, 1, LATTICE_LINES, POINTS_ACROSS), jnp.float32, -1.0, 1.0)
    flows = jnp.clip(0.1 * jax.random.normal(keys[1], (ENSEMBLE_SIZE, 2, LATTICE_LINES, POINTS_ACROSS), jnp.float32), -0.4, 0.4)
    return jnp.concatenate([depth, flows], 1).astype(jnp.float32)


def touch_ends(values, key, least, high):
    extent = values.shape
    index_at = [jax.random.randint(jax.random.fold_in(key, axis), (), 0, extent[axis]) for axis in range(len(extent))]
    values = values.at[tuple(index_at)].set(least)
    longest = extent.index(max(extent))
    index_at[longest] = (index_at[longest] + 1) % extent[longest]
    return values.at[tuple(index_at)].set(high)


def shard_levels(rng, dims, cuts, low, high):
    def one(dim, shards_of):
        heights = jax.random.uniform(jax.random.fold_in(jax.random.fold_in(rng, 6), dim), (shards_of,), jnp.float32, low / len(cuts), high / len(cuts))
        return jnp.repeat(jnp.exp(heights), dims[dim] // shards_of).reshape((-1,) + (1,) * (len(dims) - dim - 1))

    factor_of = one(*cuts[0])
    for cut in cuts[1:]:
        factor_of = factor_of * one(*cut)
    return factor_of


def gaussian(own_key, shape, scale, most, cuts=(), kind=jnp.bfloat16):
    entries = jax.random.normal(own_key, shape, jnp.float32) * scale
    if len(cuts) > 0:
        entries = shard_levels(own_key, shape, cuts, -0.22, 0.18) * entries
    return jnp.clip(entries, min=-most, max=most).astype(kind)


def setup_inputs(seed: int = 0) -> dict:
    key_of = jax.random.split(jax.random.key(seed), 7)
    return {
        "prior_fields": draw_prior_fields(jax.random.fold_in(key_of[6], 71), 0),
        "measured_point_location": touch_ends(jax.random.randint(key_of[1], (NOBS,), 0, RY * POINTS_ACROSS), jax.random.fold_in(key_of[1], 1), 0, (RY * POINTS_ACROSS) - 1).astype(jnp.int32),
        "measured_depths": jnp.clip(0.7 + 0.59999996 * jax.random.uniform(key_of[2], (NOBS,), jnp.float32) ** shard_levels(key_of[2], (NOBS,), ((0, 16),), -0.2, 0.2), 0.7, 1.3),
        "inverse_noise_deviation": jnp.clip(jnp.exp(math.log(40.0) - 2.0794415 * jax.random.uniform(key_of[3], (NOBS,), jnp.float32) ** shard_levels(key_of[3], (NOBS,), ((0, 16),), -0.2, 0.2)), 5.0, 40.0),
        "sample_noise_draw": gaussian(key_of[4], (ENSEMBLE_SIZE, NOBS), 1.0, 6.0, ((1, 16),), jnp.float32),
        "sample_line_labels": jax.random.permutation(key_of[5], ENSEMBLE_SIZE).astype(jnp.int32),
    }


gravity = 1.0
courant = 0.35
widen_dispersion = 1.1

def lax_friedrichs(state):
    depth = state[:, 0]
    east = state[:, 1]
    north = state[:, 2]
    press = 0.5 * gravity * depth * depth
    flux_x = jnp.stack([east, east * east / depth + press, east * north / depth], 1)
    flux_y = jnp.stack([north, east * north / depth, north * north / depth + press], 1)
    inner = state[:, :, 1:-1]
    average = 0.25 * (state[:, :, 2:] + state[:, :, :-2] + jnp.roll(inner, 1, 3) + jnp.roll(inner, -1, 3))
    middle = flux_x[:, :, 1:-1]
    return average - 0.5 * courant * (jnp.roll(middle, -1, 3) - jnp.roll(middle, 1, 3)) - 0.5 * courant * (flux_y[:, :, 2:] - flux_y[:, :, :-2])

def prior_strip_slab(strip_slab):
    for step in range(STEPS):
        padded = jnp.concatenate([strip_slab[:, :, -1:], strip_slab, strip_slab[:, :, :1]], 2)
        strip_slab = lax_friedrichs(padded)
    return strip_slab

def reference(prior_fields, measured_point_location, measured_depths, inverse_noise_deviation, sample_noise_draw, sample_line_labels):
    propagated_fields = lax.map(prior_strip_slab, prior_fields.reshape(ENSEMBLE_SIZE // 16, 16, 3, LATTICE_LINES, POINTS_ACROSS)).reshape(ENSEMBLE_SIZE, 3, LATTICE_LINES, POINTS_ACROSS)
    blocks = (jnp.arange(NOBS, dtype=jnp.int32) // OBS_DEV).astype(jnp.int32)
    cells = (blocks * (RY * POINTS_ACROSS) + measured_point_location).astype(jnp.int32)
    depth_flat = propagated_fields[:, 0].reshape(ENSEMBLE_SIZE, LATTICE_LINES * POINTS_ACROSS)
    sampled = inverse_noise_deviation[None, :] * depth_flat[:, cells]
    innovation = inverse_noise_deviation[None, :] * measured_depths[None, :] - sampled + sample_noise_draw[sample_line_labels]
    dispersion_multiplier = math.sqrt(widen_dispersion / (ENSEMBLE_SIZE - 1))
    spread = dispersion_multiplier * (sampled - lax.optimization_barrier(jnp.mean(sampled, axis=0, keepdims=True)))
    gram = jnp.dot(spread, spread.T, precision=lax.Precision.HIGHEST, preferred_element_type=jnp.float32)
    cross = jnp.dot(innovation, spread.T, precision=lax.Precision.HIGHEST, preferred_element_type=jnp.float32)
    upper = 1.0 + jnp.sqrt(jnp.sum(gram * gram))
    theta = (upper + 1.0) / 2.0
    delta = (upper - 1.0) / 2.0
    sigma = theta / delta
    rho = 1.0 / sigma
    residual = cross
    direction = residual / theta
    linear_solution = direction
    for turn in range(CHEB - 1):
        residual = residual - direction - jnp.dot(direction, gram, precision=lax.Precision.HIGHEST, preferred_element_type=jnp.float32)
        rho_next = 1.0 / (2.0 * sigma - rho)
        direction = rho_next * rho * direction + 2.0 * rho_next / delta * residual
        linear_solution = linear_solution + direction
        rho = rho_next
    ensemble_combination = math.sqrt(widen_dispersion) * jnp.eye(ENSEMBLE_SIZE, dtype=jnp.float32) + dispersion_multiplier * linear_solution
    flat = propagated_fields.reshape(ENSEMBLE_SIZE, 3 * LATTICE_LINES * POINTS_ACROSS)
    center = lax.optimization_barrier(jnp.mean(flat, axis=0, keepdims=True))
    result = center + jnp.dot(ensemble_combination, flat - center, precision=lax.Precision.HIGHEST, preferred_element_type=jnp.float32)
    return result.reshape(ENSEMBLE_SIZE, 3, LATTICE_LINES, POINTS_ACROSS)
```

```python
import math

import jax
import jax.numpy as jnp
from jax import lax
from jax.experimental import pallas as pl
from jax.experimental.pallas import tpu as pltpu
from jax.sharding import Mesh
from jax.sharding import PartitionSpec as P

MEMBERS = 1024
STEPS = 4
CHEB = 8
RUN = ("run_0", "run_1")
ROLE_GRP = ("role", "grp_0", "grp_1")
LINE = ("role", "grp_0")
CORE = "grp_1"

gravity = 1.0
courant = 0.35
inflate = 1.1
scale = math.sqrt(inflate / (MEMBERS - 1))


def dot3(left, right):
    return jnp.dot(left, right, precision=lax.Precision.HIGH, preferred_element_type=jnp.float32)


def forecast_kernel(above_ref, own_ref, below_ref, out_ref, a_ref, b_ref):
    rows = own_ref.shape[0]
    total = rows + 2 * STEPS

    def row_of(step, y):
        if step == 0:
            if y < STEPS:
                return [above_ref[y, k] for k in range(3)]
            if y < STEPS + rows:
                return [own_ref[y - STEPS, k] for k in range(3)]
            return [below_ref[y - STEPS - rows, k] for k in range(3)]
        ref = (b_ref, a_ref)[step % 2]
        return [ref[y, k] for k in range(3)]

    half = 0.5 * courant
    for step in range(STEPS):
        last = step == STEPS - 1

        def parts(y, step=step):
            d, p, r = row_of(step, y)
            inv = 1.0 / d
            press = (0.5 * gravity) * d * d
            u = p * inv
            fx = (p, p * u + press, r * u)
            fy = (r, r * u, r * r * inv + press)
            quarter = [0.25 * q for q in (d, p, r)]
            hx = [half * f for f in fx]
            hy = [half * f for f in fy]
            side = [
                pltpu.roll(quarter[k] - hx[k], 127, 1) + pltpu.roll(quarter[k] + hx[k], 1, 1)
                for k in range(3)
            ]
            down = [quarter[k] - hy[k] for k in range(3)]
            up = [quarter[k] + hy[k] for k in range(3)]
            return side, down, up

        window = [parts(step), parts(step + 1)]
        for y in range(step + 1, total - step - 1):
            window.append(parts(y + 1))
            before, here, after = window
            for k in range(3):
                new = here[0][k] + after[1][k] + before[2][k]
                if last:
                    out_ref[y - STEPS, k] = new
                elif step % 2 == 0:
                    a_ref[y, k] = new
                else:
                    b_ref[y, k] = new
            window = window[1:]


def forecast(above, own, below):
    rows, comps, members, width = own.shape
    block = lambda n: pl.BlockSpec((n, comps, 8, width), lambda i: (0, 0, i, 0))
    scratch = pltpu.VMEM((rows + 2 * STEPS, comps, 8, width), jnp.float32)
    return pl.pallas_call(
        forecast_kernel,
        grid=(members // 8,),
        in_specs=[block(STEPS), block(rows), block(STEPS)],
        out_specs=block(rows),
        out_shape=jax.ShapeDtypeStruct(own.shape, jnp.float32),
        scratch_shapes=[scratch, scratch],
        name="forecast",
    )(above, own, below)


def observe_kernel(stepped_ref, location_ref, depths_ref, inverse_ref, labels_ref, noise_ref, sampled_ref, innov_ref, drawn_ref):
    rows, members, width = stepped_ref.shape
    observed = location_ref.shape[1]

    def take(i, carry):
        drawn_ref[pl.ds(i, 1), :] = noise_ref[pl.ds(labels_ref[i], 1), :]
        return carry

    lax.fori_loop(0, members, take, 0)
    location = location_ref[...]
    total = jnp.zeros((members, observed), jnp.float32)
    column = lax.broadcasted_iota(jnp.int32, (width, observed), 0)
    for y in range(rows):
        chosen = jnp.where(column + y * width == location, 1.0, 0.0)
        total += jnp.dot(stepped_ref[y], chosen, precision=lax.Precision.HIGHEST, preferred_element_type=jnp.float32)
    inverse = inverse_ref[...]
    sampled = inverse * total
    sampled_ref[...] = sampled
    innov_ref[...] = inverse * depths_ref[...] - sampled + drawn_ref[...]


def observe(stepped, location, depths, inverse, labels, noise):
    rows, comps, members, width = stepped.shape
    observed = location.shape[0]
    whole = lambda *shape: pl.BlockSpec(shape, lambda i, labels: (0,) * len(shape))
    result = jax.ShapeDtypeStruct((members, observed), jnp.float32)
    return pl.pallas_call(
        lambda labels_ref, *refs: observe_kernel(*refs[:4], labels_ref, *refs[4:]),
        grid_spec=pltpu.PrefetchScalarGridSpec(
            num_scalar_prefetch=1,
            grid=(1,),
            in_specs=[
                pl.BlockSpec((rows, None, members, width), lambda i, labels: (0, 0, 0, 0)),
                whole(1, observed),
                whole(1, observed),
                whole(1, observed),
                whole(*noise.shape),
            ],
            out_specs=[whole(members, observed)] * 2,
            scratch_shapes=[pltpu.VMEM((members, observed), jnp.float32)],
        ),
        out_shape=[result, result],
        name="observe",
    )(labels, stepped, location[None], depths[None], inverse[None], noise)


def shared_along(shard, axis, count):
    return lax.all_to_all(
        jnp.broadcast_to(shard[None], (count, *shard.shape)), axis, 0, 0, tiled=True
    )


def both_cores(shard):
    other = lax.ppermute(shard, CORE, [(0, 1), (1, 0)])
    first = lax.axis_index(CORE) == 0
    return jnp.stack([jnp.where(first, shard, other), jnp.where(first, other, shard)])


def shards(prior, location, depths, inverse, noise, labels):
    members = prior.shape[0]
    runs = lax.axis_size(RUN)
    lines = lax.axis_size(LINE)
    per = members // runs
    state = prior.transpose(2, 1, 0, 3)
    below = lax.ppermute(state[:STEPS], RUN, [((i + 1) % runs, i) for i in range(runs)])
    above = lax.ppermute(state[-STEPS:], RUN, [(i, (i + 1) % runs) for i in range(runs)])
    stepped = forecast(above, state, below)
    sampled, innovation = observe(stepped, location, depths, inverse, labels, noise)

    everyone = both_cores(shared_along(sampled, LINE, lines)).reshape(MEMBERS, -1)
    stepped, everyone = lax.optimization_barrier((stepped, everyone))
    mean = jnp.mean(everyone, axis=0, keepdims=True)
    spread = scale * (everyone - mean)
    own = scale * (sampled - mean)
    left = jnp.stack([own.reshape(runs, per, -1), innovation.reshape(runs, per, -1)], 1)
    partial = lax.dot_general(
        left.reshape(2 * members, -1),
        spread,
        (((1,), (1,)), ((), ())),
        precision=lax.Precision.HIGH,
        preferred_element_type=jnp.float32,
    ).reshape(runs, 2 * per, MEMBERS)
    summed = jnp.sum(lax.all_to_all(partial, RUN, 0, 0, tiled=True), axis=0)
    lined = shared_along(summed, LINE, lines)

    def whole(rows):
        run_major = both_cores(shared_along(rows.reshape(lines * per, MEMBERS), RUN, runs))
        split = run_major.reshape(2, runs, lines, per, MEMBERS)
        return split.transpose(0, 2, 1, 3, 4).reshape(MEMBERS, MEMBERS)

    gram = whole(lined[:, :per])

    cells = lax.all_to_all(stepped, ROLE_GRP, 0, 0, tiled=True)
    width = cells.shape[-1]
    cells = cells.reshape(lines, 2, 3, members, width).transpose(1, 0, 3, 2, 4)
    flat = cells.reshape(MEMBERS, 3 * width)
    center = jnp.mean(flat, axis=0, keepdims=True)
    moved = flat - center

    upper = 1.0 + jnp.sqrt(jnp.sum(gram * gram))
    theta = (upper + 1.0) / 2.0
    delta = (upper - 1.0) / 2.0
    sigma = theta / delta
    rho = 1.0 / sigma
    residual = moved
    direction = residual / theta
    solved = direction
    for turn in range(CHEB - 1):
        residual = residual - direction - dot3(gram, direction)
        rho_next = 1.0 / (2.0 * sigma - rho)
        direction = rho_next * rho * direction + 2.0 * rho_next / delta * residual
        solved = solved + direction
        rho = rho_next
    late, gram = lax.optimization_barrier((lined[:, per:], gram))
    cross = whole(late)
    updated = center + math.sqrt(inflate) * moved + scale * dot3(cross, solved)
    parcels = updated.reshape(2, lines, members, 3, width).transpose(1, 0, 3, 2, 4)
    parcels = parcels.reshape(2 * lines, 3, members, width)
    home = lax.all_to_all(parcels, ROLE_GRP, 0, 0, tiled=True)
    return home.transpose(2, 1, 0, 3)


def solution(mesh):
    torus = Mesh(
        mesh.devices.reshape(mesh.shape["role"], 2, 2, 4, 4),
        ("role", "grp_0", "grp_1", "run_0", "run_1"),
    )
    placed = (P(ROLE_GRP, None, RUN, None), P(RUN), P(RUN), P(RUN), P(None, RUN), P(ROLE_GRP))
    return jax.shard_map(
        shards, mesh=torus, in_specs=placed, out_specs=P(ROLE_GRP, None, RUN, None), check_vma=False
    )
```
